32 devices in a mesh: dp: 2 (over x), tp: 16 (over y, z, core).
Axes of the slice: x: 2, y: 2, z: 4, core: 2. Of those that a mesh axis runs over, the one named last changes fastest.
Arguments:
- x: bfloat16 [8192, 4096], P(('dp', 'tp')), parts along dimension 0
- dy: bfloat16 [8192, 4096], P(('dp', 'tp')), parts along dimension 0
- gate: bfloat16 [8192, 14336], P('dp', 'tp'), parts along dimension 0
- up: bfloat16 [8192, 14336], P('dp', 'tp'), parts along dimension 0
- w_gate: bfloat16 [4096, 14336], P(None, 'tp')
- w_up: bfloat16 [4096, 14336], P(None, 'tp')
- w_down: bfloat16 [14336, 4096], P('tp')
Outputs:
- output 1: bfloat16 [8192, 4096], P(('dp', 'tp')), parts along dimension 0
- output 2: bfloat16 [8192, 14336], P('dp', 'tp'), parts along dimension 0
- output 3: bfloat16 [8192, 14336], P('dp', 'tp'), parts along dimension 0
- output 4: bfloat16 [28672, 4096], P(('dp', 'tp')), parts along dimension 0
There are 2 independent parts. The reference program is written for one: setup_inputs(seed, part) draws one part's arguments, and reference() takes and returns one part's arrays. A program takes and returns all parts, laid end to end along the dimension named above; an argument that names none is the same for every part.
All inputs are finite; a program needn't handle non-finite values.
Results may differ from the reference program's by a relative error of at most 0.012.
Values are sent between devices in bfloat16 or wider.
A program may use at most 2 GiB of HBM per device.

```python
import jax
import jax.numpy as jnp

ROWS = 4096
D = 4096
FF = 14336


def act(gate, up):
    return jax.nn.silu(gate) * up


def setup_inputs(seed: int = 0, part: int = 0) -> dict:
    kx, ky, ka, kb, kg, ku, kd = jax.random.split(jax.random.key(seed), 7)
    kx, ky, ka, kb = (jax.random.fold_in(k, part) for k in (kx, ky, ka, kb))
    drawn = {
        "x": jax.random.normal(kx, (ROWS, D), jnp.float32),
        "dy": jax.random.normal(ky, (ROWS, D), jnp.float32),
        "gate": jax.random.normal(ka, (ROWS, FF), jnp.float32),
        "up": jax.random.normal(kb, (ROWS, FF), jnp.float32),
        "w_gate": jax.random.normal(kg, (D, FF), jnp.float32) * D**-0.5,
        "w_up": jax.random.normal(ku, (D, FF), jnp.float32) * D**-0.5,
        "w_down": jax.random.normal(kd, (FF, D), jnp.float32) * FF**-0.5,
    }
    return {k: v.astype(jnp.bfloat16) for k, v in drawn.items()}


def reference(x, dy, gate, up, w_gate, w_up, w_down):
    hidden, back = jax.vjp(act, gate.astype(jnp.float32), up.astype(jnp.float32))
    d_hidden = jnp.dot(dy, w_down.T, preferred_element_type=jnp.float32)
    d_gate, d_up = (g.astype(jnp.bfloat16) for g in back(d_hidden))
    dx = jnp.dot(d_gate, w_gate.T, preferred_element_type=jnp.float32) + jnp.dot(d_up, w_up.T, preferred_element_type=jnp.float32)
    dw_gate = jnp.dot(x.T, d_gate, preferred_element_type=jnp.float32)
    dw_up = jnp.dot(x.T, d_up, preferred_element_type=jnp.float32)
    dw_down = jnp.dot(hidden.astype(jnp.bfloat16).T, dy, preferred_element_type=jnp.float32)
    return tuple(g.astype(jnp.bfloat16) for g in (dx, dw_gate, dw_up, dw_down))
```

```python
import jax
import jax.numpy as jnp
from jax import lax
from jax.experimental import pallas as pl
from jax.experimental.pallas import tpu as pltpu
from jax.sharding import PartitionSpec as P

BF, F32 = jnp.bfloat16, jnp.float32
LIMIT = 67043328
R, D, C = 256, 4096, 896
HB, HN = R // 2, D // 2
NB = 16
W, WP = 512, 256
QA = 12
NT, TT = (((1,), (1,)), ((), ())), (((0,), (0,)), ((), ()))
DY, X = 0, 1

LINKS = {
    "C": {
        "in": "d000d001x000x001",
        "out": "",
        "y": "d000d001d100d101d200d201d300x000x001x100x101x200x201x300x301",
    },
    "M": {
        "in": "d100d101d000d001x100d011x101x000x001",
        "out": "d100d101d200d201d300d301x100d311x101x200x201x300x301",
        "y": "d100d101d000d001d200d201d300x100x101x000x001x200x201x300x301",
    },
}
OWN = {"C": 0, "M": 1}
NONE, T1, T2P, T2O, DWD, P1 = range(6)
TASKS = {
    "C": (
        ("t000t001p001", "", "t100t010t101t011", "p101p011", "t110t111p111o00-o01-", "t200t201p201", "t300t301p301o10-o11-",
         "t210t211p211", "t310t311p311o20-o21-"),
        ("d03-", "o30-o31-d35-", "d58-", "o40-o41-", "x04-", "o50-o51-x48-o60-", "o61-x8c-", "xcg-", "o70-o71-"),
    ),
    "M": (
        ("t100t101p101", "", "t000t200t110t001", "t201t111p001", "t300t010t301t011", "p301p201p111", "t210t211p211p011", "",
         "t310t311p311o00-"),
        ("o01-d02-", "d24-o10-", "o11-d46-", "o20-o30-d68-", "o21-o31-x04-", "o40-o60-x48-o50-", "o41-o61-o51-x8c-", "xcg-", "o70-o71-"),
    ),
}
IN, OUT, Y, HERE = range(4)
SUMS = {
    "C": ("1100I", "3000I", "3100I", "2100I", "2000I", "1000I", "0101Y", "0001H"),
    "M": ("3010I", "3110I", "2110I", "0101O", "2010I", "0001O", "1111Y", "1011H"),
}


def fours(text):
    return [text[n:n + 4] for n in range(0, len(text), 4)]


def parse(token):
    return ("dx".index(token[0]), *map(int, token[1:]))


def services(kind):
    waits, sends = {}, {}
    arrivals = [(s, parse(e)) for s, e in enumerate(fours(LINKS["M" if kind == "C" else "C"]["out" if kind == "C" else "in"]))]
    if kind == "M":
        for s, e in enumerate(fours(LINKS["M"]["in"])):
            a, p, yr, h = parse(e)
            arrivals.append((s, (a, 3 - p, yr, h)))
    for s, e in enumerate(fours(LINKS[kind]["y"])):
        a, p, _, h = parse(e)
        arrivals.append((s, (a, p, 1, h)))
    for s, e in arrivals:
        waits.setdefault(s + 1, []).append(e)
        sends.setdefault(s + 1, []).append((*e, "d2d"))
    for link in ("in", "out", "y"):
        for s, e in enumerate(fours(LINKS[kind][link])):
            sends.setdefault(max(s - 1, 0), []).append((*parse(e), link))
    for a in (DY, X):
        for h in range(2):
            sends.setdefault(a, []).append((a, OWN[kind], 0, h, "d2d"))
    return waits, sends


def steps_of(kind, phase):
    out, slot = [], 0
    for text in TASKS[kind][phase]:
        mine, tokens = [], fours(text)
        for n, e in enumerate(tokens):
            what = 1 + "tpodx".index(e[0])
            if what <= T2P:
                q = [8 * int(f[2]) + 2 * int(f[1]) + int(f[3]) if f[0] == "t" else -1 for f in (tokens[n - 1] if n else "-", e, (tokens + ["-"])[n + 1])]
                if what == T1:
                    mine.append((T1, q[1], (q[0] >= 0) + 2 * slot + 4 * (q[2] + 1)))
                    slot = 1 - slot
                else:
                    mine.append((T2P, 8 * int(e[2]) + 2 * int(e[1]) + int(e[3]), 0))
            else:
                mine.append((what, int(e[1], 17), int(e[2], 17)))
        out.append(mine)
    return out


def table(i, values):
    out = jnp.int32(values[0])
    for n in range(1, len(values)):
        if values[n] != values[n - 1]:
            out = jnp.where(i >= n, jnp.int32(values[n]), out)
    return out


def gather_cols(src, where, q0, count, m, w, buf, s, sems):
    @pl.loop(0, count)
    def _(k):
        b, _ = where(q0 + k)
        pltpu.make_async_copy(
            src.at[pl.ds(pl.multiple_of(b * R, R), R), pl.ds(pl.multiple_of(m * w, w), w)],
            buf.at[s, pl.ds(pl.multiple_of(k * R, R), R), :], sems.at[s]).start()


def chunks(lo, hi, start, wait, work, out_start, out_wait):
    start(lo, lo % 2)

    @pl.loop(lo, hi)
    def _(m):
        s = m % 2

        @pl.when(m + 1 < hi)
        def _():
            start(m + 1, 1 - s)

        wait(s)

        @pl.when(m >= lo + 2)
        def _():
            out_wait(s)

        work(m, s)
        out_start(m, s)

    @pl.when(hi - lo >= 2)
    def _():
        out_wait(hi % 2)

    out_wait((hi - 1) % 2)


def kernel(x_ref, dy_ref, gate_ref, up_ref, wg_ref, wu_ref, wd_ref,
           part_ref, dgq_ref, dwd_ref, dyg, xg, rsb, pb, yb, accb,
           wgu, dgu, ht, out_z, acc, inc,
           ag_recv, ag_send, rs_recv, pb_recv, yb_recv, od_send, oz_send, ld, slot_in, slot_out):
    g, t = lax.axis_index("dp"), lax.axis_index("tp")
    y, z, c = t // 8, (t // 2) % 4, t % 2
    far = z // 2
    sigma, base = 1 - 2 * far, 3 * far
    corner = 1 - ((z + 1) // 2) % 2
    is_c = corner == 1
    kinds = {"C": is_c, "M": corner == 0}
    zin, zout = z + sigma, lax.rem(z - sigma + 4, 4)
    full = (dyg, xg)
    own_in = (dy_ref, x_ref)

    def dev(yy, zz, cc):
        return (g, yy * 8 + zz * 2 + cc)

    def place(p, yr):
        return y + yr * (1 - 2 * y), base + sigma * p

    def where(q):
        yy, zz = place((q % 8) // 2, q // 8)
        cr = q % 2
        return yy * 8 + zz * 2 + c + cr * (1 - 2 * c), yy * 4 + zz

    targets = {"in": dev(y, zin, c), "out": dev(y, zout, c), "y": dev(1 - y, z, c), "d2d": dev(y, z, 1 - c)}

    def half(ref, b, h):
        return ref.at[pl.ds(pl.multiple_of(b * R + h * HB, HB), HB), :]

    def block(ref, b):
        return ref.at[pl.ds(pl.multiple_of(b * R, R), R), :]

    barrier = pltpu.get_barrier_semaphore()
    for name in ("in", "y", "d2d"):
        pl.semaphore_signal(barrier, inc=1, device_id=targets[name], device_id_type=pl.DeviceIdType.MESH)

    @pl.when(corner == 0)
    def _():
        pl.semaphore_signal(barrier, inc=1, device_id=targets["out"], device_id_type=pl.DeviceIdType.MESH)

    pl.semaphore_wait(barrier, 4 - corner)

    def ag_copy(a, p, yr, h, link, own):
        yy, zz = place(p, yr)
        b = yy * 8 + zz * 2 + c
        src = own_in[a].at[pl.ds(h * HB, HB), :] if own else half(full[a], b, h)
        return pltpu.make_async_remote_copy(
            src_ref=src, dst_ref=half(full[a], b, h), send_sem=ag_send.at[a, 0 if link in ("in", "out") else 1],
            recv_sem=ag_recv.at[a, b, h], device_id=targets[link], device_id_type=pl.DeviceIdType.MESH)

    def arrived(a, b, h):
        pltpu.make_async_copy(half(full[a], b, h), half(full[a], b, h), ag_recv.at[a, b, h]).wait()

    def service(kind, waits, sends):
        for a, p, yr, h in waits:
            yy, zz = place(p, yr)
            arrived(a, yy * 8 + zz * 2 + c, h)
        for a, p, yr, h, link in sends:
            ag_copy(a, p, yr, h, link, own=(p == OWN[kind] and yr == 0)).start()

    plans = {kind: services(kind) for kind in ("C", "M")}

    def task_t1(q, code, wd, dyb, gb, ub):
        loaded, slot, after = code % 2, (code // 2) % 2, code // 4 - 1

        def loads(q, s):
            b, _ = where(q)
            return (pltpu.make_async_copy(block(dyg, b), dyb.at[s], ld.at[s]),
                    pltpu.make_async_copy(block(gate_ref, b), gb.at[s], ld.at[2 + s]),
                    pltpu.make_async_copy(block(up_ref, b), ub.at[s], ld.at[4 + s]))

        def start(q, s):
            @pl.when(q % 2 == 1)
            def _():
                for h in range(2):
                    arrived(DY, where(q)[0], h)

            for cp in loads(q, s):
                cp.start()

        @pl.when(loaded == 0)
        def _():
            start(q, slot)

        @pl.when(after >= 0)
        def _():
            start(after, 1 - slot)

        here = loads(q, slot)
        here[0].wait()
        acc[:, :C] = lax.dot_general(dyb[slot], wd[...], NT, preferred_element_type=F32)
        for cp in here[1:]:
            cp.wait()
        rc = 32

        @pl.loop(0, R // rc)
        def _(r):
            rs = pl.ds(pl.multiple_of(r * rc, rc), rc)
            to = pl.ds(pl.multiple_of(q * R + r * rc, rc), rc)
            dh, gg, uu = acc[rs, :C], gb[slot, rs, :].astype(F32), ub[slot, rs, :].astype(F32)
            s = jax.nn.sigmoid(gg)
            silu = gg * s
            acc[rs, C:2 * C] = silu * uu
            dgu[to, C:] = (dh * silu).astype(BF)
            dgu[to, :C] = ((dh * uu) * (s * (1.0 + gg * (1.0 - s)))).astype(BF)

        ht[:, pl.ds(pl.multiple_of(q * R, R), R)] = acc[:, C:2 * C].T.astype(BF)

    def product(q, n):
        lhs = dgu[pl.ds(pl.multiple_of(q * R, R), R), :]
        return lax.dot_general(lhs, wgu[pl.ds(pl.multiple_of(n * HN, HN), HN), :], NT, preferred_element_type=F32)

    def cols_of(n):
        return pl.ds(pl.multiple_of(n * HN, HN), HN)

    def od_copy(out_d, u, n):
        return pltpu.make_async_remote_copy(
            src_ref=out_d.at[n], dst_ref=pb.at[u, :, cols_of(n)], send_sem=od_send.at[n], recv_sem=pb_recv.at[u, n],
            device_id=targets["d2d"], device_id_type=pl.DeviceIdType.MESH)

    def task_t2p(q, first, out_d):
        _, u = where(q)

        @pl.loop(0, 2)
        def _(n):
            @pl.when(first == 0)
            def _():
                od_copy(out_d, u, n).wait_send()

            out_d[n] = product(q, n).astype(BF)
            od_copy(out_d, u, n).start()

    def oz_copy(j, n, u, to, dirn):
        return pltpu.make_async_remote_copy(
            src_ref=out_z.at[j % 3, n], dst_ref=rsb.at[dirn, u, :, cols_of(n)], send_sem=oz_send.at[j % 3, n],
            recv_sem=rs_recv.at[dirn, u, n], device_id=dev(y, to, c), device_id_type=pl.DeviceIdType.MESH)

    def y_copy(j, n):
        return pltpu.make_async_remote_copy(
            src_ref=out_z.at[j % 3, n], dst_ref=yb.at[:, cols_of(n)], send_sem=oz_send.at[j % 3, n],
            recv_sem=yb_recv.at[n], device_id=targets["y"], device_id_type=pl.DeviceIdType.MESH)

    def task_t2o(j, n):
        def pick(col, names):
            return jnp.where(is_c, *(table(j, [names.index(e[col]) for e in SUMS[kind]]) for kind in ("C", "M")))

        p, yr, fo, fi = (pick(col, "0123") for col in range(4))
        dest = pick(4, "IOYH")
        q = 8 * yr + 2 * p
        _, u = where(q)
        cs = cols_of(n)
        sources = (
            (jnp.int32(1), pb.at[u, :, cs], pb_recv.at[u, n]),
            (fo, rsb.at[0, u, :, cs], rs_recv.at[0, u, n]),
            (fi, rsb.at[1, u, :, cs], rs_recv.at[1, u, n]),
        )

        def fetch(s):
            flag, ref, sem = sources[s]

            @pl.when(flag == 1)
            def _():
                pltpu.make_async_copy(ref, ref, sem).wait()
                pltpu.make_async_copy(ref, inc.at[s], ld.at[s]).start()

        early = jnp.where((corner == 0) | (j >= 3) | (n == 1), 1, 0)

        @pl.when(early == 1)
        def _():
            fetch(0)

        acc[...] = product(q, n)

        @pl.when(early == 0)
        def _():
            fetch(0)

        fetch(1)
        fetch(2)
        for s, (flag, ref, sem) in enumerate(sources):
            @pl.when(flag == 1)
            def _():
                pltpu.make_async_copy(ref, inc.at[s], ld.at[s]).wait()
                acc[...] += inc[s].astype(F32)

        @pl.when(dest < HERE)
        def _():
            @pl.when(j >= 3)
            def _():
                y_copy(j, n).wait_send()

            out_z[j % 3, n] = acc[...].astype(BF)

        @pl.when(dest < Y)
        def _():
            oz_copy(j, n, u, jnp.where(dest == IN, zin, zout), jnp.where(dest == IN, 1 - corner, 1)).start()

        @pl.when(dest == Y)
        def _():
            y_copy(j, n).start()

        @pl.when(dest == HERE)
        def _():
            done = pltpu.make_async_copy(acc, part_ref.at[:, cs], ld.at[0])
            done.start()
            done.wait()

    def gather(src, q0, count, m, w, buf, s):
        gather_cols(src, where, q0, count, m, w, buf, s, slot_in)

    def task_dwd(lo, hi):
        def body(buf, out):
            def out_copy(m, s):
                return pltpu.make_async_copy(out.at[s], dwd_ref.at[:, pl.ds(pl.multiple_of(m * W, W), W)], slot_out.at[s])

            def work(m, s):
                out[s] = jnp.dot(ht[...], buf[s], preferred_element_type=F32).astype(BF)

            chunks(lo, hi, lambda m, s: gather(dyg, 0, NB, m, W, buf, s),
                   lambda s: pltpu.make_async_copy(buf.at[s], buf.at[s], slot_in.at[s]).wait(), work,
                   lambda m, s: out_copy(m, s).start(), lambda s: out_copy(0, s).wait())

        pl.run_scoped(body, pltpu.VMEM((2, NB * R, W), BF), pltpu.VMEM((2, C, W), BF))

    def x_arrived(q0, count):
        @pl.loop(0, count)
        def _(k):
            b, _ = where(q0 + 2 * k + 1)
            for h in range(2):
                arrived(X, b, h)

    def task_p1(lo, hi):
        @pl.when(lo == 0)
        def _():
            x_arrived(0, 6)

        def body(buf, out):
            def out_copy(m, s):
                return pltpu.make_async_copy(out.at[s], accb.at[pl.ds(pl.multiple_of(m * WP, WP), WP), :], slot_out.at[s])

            def work(m, s):
                out[s] = lax.dot_general(buf[s], dgu[:QA * R, :], TT, preferred_element_type=F32)

            chunks(lo, hi, lambda m, s: gather(xg, 0, QA, m, WP, buf, s),
                   lambda s: pltpu.make_async_copy(buf.at[s], buf.at[s], slot_in.at[s]).wait(), work,
                   lambda m, s: out_copy(m, s).start(), lambda s: out_copy(0, s).wait())

        pl.run_scoped(body, pltpu.VMEM((2, QA * R, WP), BF), pltpu.VMEM((2, WP, 2 * C), F32))

    def run(phase, handlers):
        steps, at = {"C": [], "M": []}, {}
        points = {kind: steps_of(kind, phase) for kind in steps}
        for n, lists in enumerate(zip(points["C"], points["M"])):
            count = max(1, *map(len, lists))
            at[n + phase * len(TASKS["C"][0])] = len(steps["C"])
            for kind, mine in zip(("C", "M"), lists):
                steps[kind] += mine + [(NONE, 0, 0)] * (count - len(mine))

        @pl.loop(0, len(steps["C"]))
        def _(i):
            for k, start in at.items():
                for kind, mine in kinds.items():
                    waits, sends = (e.get(k, []) for e in plans[kind])
                    if k and (waits or sends):
                        @pl.when((i == start) & mine)
                        def _():
                            service(kind, waits, sends)

            what, a1, a2 = (
                jnp.where(is_c, table(i, [e[col] for e in steps["C"]]), table(i, [e[col] for e in steps["M"]])) for col in range(3))
            for kind, fn in handlers.items():
                @pl.when(what == kind)
                def _():
                    fn(i, a1, a2)

    def phase_one(wd, dyb, gb, ub, out_d):
        for kind, mine in kinds.items():
            @pl.when(mine)
            def _():
                service(kind, *(e.get(0, []) for e in plans[kind]))

        weights = [
            pltpu.make_async_copy(wd_ref, wd, ld.at[3]),
            pltpu.make_async_copy(wg_ref, wgu.at[:, pl.ds(0, C)], ld.at[4]),
            pltpu.make_async_copy(wu_ref, wgu.at[:, pl.ds(C, C)], ld.at[5]),
        ]
        for cp in weights:
            cp.start()
        for a in (DY, X):
            for cp in (pltpu.make_async_copy(own_in[a], dyb.at[0], ld.at[0]), pltpu.make_async_copy(dyb.at[0], block(full[a], t), ld.at[0])):
                cp.start()
                cp.wait()
        for cp in weights:
            cp.wait()
        run(0, {
            T1: lambda i, q, code: task_t1(q, code, wd, dyb, gb, ub),
            T2P: lambda i, q, _: task_t2p(q, jnp.where(i < 3, 1, 0), out_d),
            T2O: lambda i, j, n: task_t2o(j, n),
        })
        for n in range(2):
            od_copy(out_d, 0, n).wait_send()

    pl.run_scoped(phase_one, pltpu.VMEM((C, D), BF), pltpu.VMEM((2, R, D), BF), pltpu.VMEM((2, R, C), BF), pltpu.VMEM((2, R, C), BF),
                  pltpu.VMEM((2, R, HN), BF))
    rest = pltpu.make_async_copy(dgu.at[pl.ds(QA * R, (NB - QA) * R), :], dgq_ref, ld.at[6])
    rest.start()
    run(1, {
        T2O: lambda i, j, n: task_t2o(j, n),
        DWD: lambda i, lo, hi: task_dwd(lo, hi),
        P1: lambda i, lo, hi: task_p1(lo, hi),
    })
    rest.wait()
    x_arrived(QA, (NB - QA) // 2)
    for n in range(2):
        pltpu.make_async_copy(yb.at[:, cols_of(n)], yb.at[:, cols_of(n)], yb_recv.at[n]).wait()
        for j in range(3):
            y_copy(j, n).wait_send()
    for kind, mine in kinds.items():
        @pl.when(mine)
        def _():
            sent = [e for es in plans[kind][1].values() for e in es]
            for a in (DY, X):
                for group, links in enumerate((("in", "out"), ("y", "d2d"))):
                    part = full[a].at[pl.ds(0, HB * sum(e[0] == a and e[4] in links for e in sent)), :]
                    pltpu.make_async_copy(part, part, ag_send.at[a, group]).wait()


def finish(part_ref, yb, accb, xg, dgq_ref, dwd_in, dx_ref, dwg_ref, dwu_ref, dwd_ref,
           dgq, buf, part, out, mine, theirs, done, rows, slot_in, acc_in, slot_out, ld, row_in, row_out):
    t = lax.axis_index("tp")
    y, z, c = t // 8, (t // 2) % 4, t % 2
    far = z // 2
    H = C * W // D

    def where(q):
        yr, p, cr = q // 8, (q % 8) // 2, q % 2
        return (y + yr * (1 - 2 * y)) * 8 + (3 * far + (1 - 2 * far) * p) * 2 + c + cr * (1 - 2 * c), 0

    loads = [pltpu.make_async_copy(a, b, ld.at[n]) for n, (a, b) in enumerate(((dgq_ref, dgq), (part_ref, mine), (yb, theirs)))]
    dx = pltpu.make_async_copy(done, dx_ref, ld.at[3])
    chunks = D // W

    def row(ref, m):
        return ref.at[pl.ds(pl.multiple_of(m * H, H), H), :]

    def ins(m, s):
        return (pltpu.make_async_copy(accb.at[pl.ds(pl.multiple_of(m * W, W), W), :], part.at[s], acc_in.at[s]),
                pltpu.make_async_copy(row(dwd_in, m), rows.at[m % 5], row_in.at[s]))

    def start(m):
        gather_cols(xg, where, QA, NB - QA, m, W, buf, m % 3, slot_in)
        for cp in ins(m, m % 3):
            cp.start()

    def outs(m):
        s, to = m % 2, pl.ds(pl.multiple_of(m * W, W), W)
        return (pltpu.make_async_copy(out.at[s, 0], dwg_ref.at[to, :], slot_out.at[s, 0]),
                pltpu.make_async_copy(out.at[s, 1], dwu_ref.at[to, :], slot_out.at[s, 1]),
                pltpu.make_async_copy(rows.at[m % 5], row(dwd_ref, m), row_out.at[s]))

    loads[0].start()
    for m in range(2):
        start(m)
    for cp in loads[1:]:
        cp.start()
    loads[0].wait()

    @pl.loop(0, chunks)
    def _(m):
        s = m % 3

        @pl.when(m + 2 < chunks)
        def _():
            start(m + 2)

        pltpu.make_async_copy(buf.at[s], buf.at[s], slot_in.at[s]).wait()
        for cp in ins(m, s):
            cp.wait()

        @pl.when(m >= 2)
        def _():
            for cp in outs(m - 2):
                cp.wait()

        total = part[s] + lax.dot_general(buf[s], dgq[...], TT, preferred_element_type=F32)
        out[m % 2, 0] = total[:, :C].astype(BF)
        out[m % 2, 1] = total[:, C:].astype(BF)
        for cp in outs(m):
            cp.start()

        @pl.when(m == 2)
        def _():
            for cp in loads[1:]:
                cp.wait()
            done[...] = (mine[...] + theirs[...].astype(F32)).astype(BF)
            dx.start()

    for m in range(2):
        for cp in outs(chunks - 2 + m):
            cp.wait()
    dx.wait()


def solution(mesh):
    def step(x, dy, gate, up, w_gate, w_up, w_down):
        hbm = pl.BlockSpec(memory_space=pl.ANY)
        S = jax.ShapeDtypeStruct
        dma = pltpu.SemaphoreType.DMA
        part, dgq, dwd, _, xg, _, _, yb, accb = pl.pallas_call(
            kernel,
            out_shape=[
                S((R, D), F32), S(((NB - QA) * R, 2 * C), BF), S((C, D), BF),
                S((NB * R, D), BF), S((NB * R, D), BF), S((2, 8, R, D), BF), S((8, R, D), BF), S((R, D), BF),
                S((D, 2 * C), F32),
            ],
            in_specs=[hbm] * 7,
            out_specs=[hbm] * 9,
            scratch_shapes=[
                pltpu.VMEM((D, 2 * C), BF),
                pltpu.VMEM((NB * R, 2 * C), BF),
                pltpu.VMEM((C, NB * R), BF),
                pltpu.VMEM((3, 2, R, HN), BF),
                pltpu.VMEM((R, HN), F32),
                pltpu.VMEM((3, R, HN), BF),
                dma((2, NB, 2)), dma((2, 2)), dma((2, 8, 2)), dma((8, 2)), dma((2,)), dma((2,)), dma((3, 2)), dma((7,)), dma((2,)),
                dma((2,)),
            ],
            compiler_params=pltpu.CompilerParams(collective_id=0, has_side_effects=True, vmem_limit_bytes=LIMIT),
            name="gather_and_sum",
        )(x, dy, gate, up, w_gate, w_up, w_down)
        return pl.pallas_call(
            finish,
            out_shape=[S((R, D), BF), S((D, C), BF), S((D, C), BF), S((C, D), BF)],
            in_specs=[hbm] * 6,
            out_specs=[hbm] * 4,
            scratch_shapes=[
                pltpu.VMEM(((NB - QA) * R, 2 * C), BF),
                pltpu.VMEM((3, (NB - QA) * R, W), BF),
                pltpu.VMEM((3, W, 2 * C), F32),
                pltpu.VMEM((2, 2, W, C), BF),
                pltpu.VMEM((R, D), F32),
                pltpu.VMEM((R, D), BF),
                pltpu.VMEM((R, D), BF),
                pltpu.VMEM((5, C * W // D, D), BF),
                dma((3,)), dma((3,)), dma((2, 2)), dma((4,)), dma((3,)), dma((2,)),
            ],
            compiler_params=pltpu.CompilerParams(vmem_limit_bytes=LIMIT),
            name="finish",
        )(part, yb, accb, xg, dgq, dwd)

    rows, cols = P(("dp", "tp"), None), P("dp", "tp")
    return jax.shard_map(
        step,
        mesh=mesh,
        in_specs=(rows, rows, cols, cols, P(None, "tp"), P(None, "tp"), P("tp", None)),
        out_specs=(rows, cols, cols, rows),
        check_vma=False,
    )
```

```python
import jax
import jax.numpy as jnp
from jax import lax
from jax.experimental import pallas as pl
from jax.experimental.pallas import tpu as pltpu
from jax.sharding import PartitionSpec as P

BF, F32 = jnp.bfloat16, jnp.float32
LIMIT = 67043328
R, D, C = 256, 4096, 896
HB, HN = R // 2, D // 2
NB = 16
W, WP = 512, 256
DE = 2560
QA = 12
NT, TT = (((1,), (1,)), ((), ())), (((0,), (0,)), ((), ()))
DY, X = 0, 1

LINKS = {
    "C": {
        "in": "d000d001x000x001",
        "out": "",
        "y": "d000d001d100d101d200d201d300x000x001x100x101x200x201x300x301",
    },
    "M": {
        "in": "d100d101d000d001x100d011x101x000x001",
        "out": "d100d101d200d201d300d301x100d311x101x200x201x300x301",
        "y": "d100d101d000d001d200d201d300x100x101x000x001x200x201x300x301",
    },
}
OWN = {"C": 0, "M": 1}
NONE, T1, T2P, T2O, DWD, P1, P3 = range(7)
TASKS = {
    "C": (
        ("t000t001p001", "", "t100t010t101t011", "p101p011", "t110t111p111o00-o01-", "t200t201p201", "t300t301p301o10-o11-",
         "t210t211p211", "t310t311p311o20-o21-"),
        ("d03-", "o30-o31-d35-", "d58-", "o40-o41-", "x04-", "o50-o51-x48-o60-", "o61-x8a-zac-", "zcg-", "o70-o71-"),
    ),
    "M": (
        ("t100t101p101", "", "t000t200t110t001", "t201t111p001", "t300t010t301t011", "p301p201p111", "t210t211p211p011", "",
         "t310t311p311o00-"),
        ("o01-d03-", "d35-o10-", "o11-d58-", "o20-o30-x03-", "o21-o31-x37-", "o40-o60-o50-x7a-", "o41-o61-o51-zac-", "zcg-", "o70-o71-"),
    ),
}
IN, OUT, Y, HERE = range(4)
SUMS = {
    "C": ("1100I", "3000I", "3100I", "2100I", "2000I", "1000I", "0101Y", "0001H"),
    "M": ("3010I", "3110I", "2110I", "0101O", "2010I", "0001O", "1111Y", "1011H"),
}


def fours(text):
    return [text[n:n + 4] for n in range(0, len(text), 4)]


def parse(token):
    return ("dx".index(token[0]), *map(int, token[1:]))


def services(kind):
    waits, sends = {}, {}
    arrivals = [(s, parse(e)) for s, e in enumerate(fours(LINKS["M" if kind == "C" else "C"]["out" if kind == "C" else "in"]))]
    if kind == "M":
        for s, e in enumerate(fours(LINKS["M"]["in"])):
            a, p, yr, h = parse(e)
            arrivals.append((s, (a, 3 - p, yr, h)))
    for s, e in enumerate(fours(LINKS[kind]["y"])):
        a, p, _, h = parse(e)
        arrivals.append((s, (a, p, 1, h)))
    for s, e in arrivals:
        waits.setdefault(s + 1, []).append(e)
        sends.setdefault(s + 1, []).append((*e, "d2d"))
    for link in ("in", "out", "y"):
        for s, e in enumerate(fours(LINKS[kind][link])):
            sends.setdefault(max(s - 1, 0), []).append((*parse(e), link))
    for a in (DY, X):
        for h in range(2):
            sends.setdefault(a, []).append((a, OWN[kind], 0, h, "d2d"))
    return waits, sends


def steps_of(kind, phase):
    out, slot = [], 0
    for text in TASKS[kind][phase]:
        mine, tokens = [], fours(text)
        for n, e in enumerate(tokens):
            what = 1 + "tpodxz".index(e[0])
            if what <= T2P:
                q = [8 * int(f[2]) + 2 * int(f[1]) + int(f[3]) if f[0] == "t" else -1 for f in (tokens[n - 1] if n else "-", e, (tokens + ["-"])[n + 1])]
                if what == T1:
                    mine.append((T1, q[1], (q[0] >= 0) + 2 * slot + 4 * (q[2] + 1)))
                    slot = 1 - slot
                else:
                    mine.append((T2P, 8 * int(e[2]) + 2 * int(e[1]) + int(e[3]), 0))
            else:
                mine.append((what, int(e[1], 17), int(e[2], 17)))
        out.append(mine)
    return out


def table(i, values):
    out = jnp.int32(values[0])
    for n in range(1, len(values)):
        if values[n] != values[n - 1]:
            out = jnp.where(i >= n, jnp.int32(values[n]), out)
    return out


def gather_cols(src, where, q0, count, m, w, buf, s, sems):
    @pl.loop(0, count)
    def _(k):
        b, _ = where(q0 + k)
        pltpu.make_async_copy(
            src.at[pl.ds(pl.multiple_of(b * R, R), R), pl.ds(pl.multiple_of(m * w, w), w)],
            buf.at[s, pl.ds(pl.multiple_of(k * R, R), R), :], sems.at[s]).start()


def chunks(lo, hi, start, wait, work, out_start, out_wait):
    start(lo, lo % 2)

    @pl.loop(lo, hi)
    def _(m):
        s = m % 2

        @pl.when(m + 1 < hi)
        def _():
            start(m + 1, 1 - s)

        wait(s)

        @pl.when(m >= lo + 2)
        def _():
            out_wait(s)

        work(m, s)
        out_start(m, s)

    @pl.when(hi - lo >= 2)
    def _():
        out_wait(hi % 2)

    out_wait((hi - 1) % 2)


def kernel(x_ref, dy_ref, gate_ref, up_ref, wg_ref, wu_ref, wd_ref,
           part_ref, dgq_ref, dwd_ref, late_ref, dyg, xg, rsb, pb, yb, accb,
           wgu, dgu, ht, out_z, acc, inc,
           ag_recv, ag_send, rs_recv, pb_recv, yb_recv, od_send, oz_send, ld, slot_in, slot_out):
    g, t = lax.axis_index("dp"), lax.axis_index("tp")
    y, z, c = t // 8, (t // 2) % 4, t % 2
    far = z // 2
    sigma, base = 1 - 2 * far, 3 * far
    corner = 1 - ((z + 1) // 2) % 2
    is_c = corner == 1
    kinds = {"C": is_c, "M": corner == 0}
    zin, zout = z + sigma, lax.rem(z - sigma + 4, 4)
    full = (dyg, xg)
    own_in = (dy_ref, x_ref)

    def dev(yy, zz, cc):
        return (g, yy * 8 + zz * 2 + cc)

    def place(p, yr):
        return y + yr * (1 - 2 * y), base + sigma * p

    def where(q):
        yy, zz = place((q % 8) // 2, q // 8)
        cr = q % 2
        return yy * 8 + zz * 2 + c + cr * (1 - 2 * c), yy * 4 + zz

    targets = {"in": dev(y, zin, c), "out": dev(y, zout, c), "y": dev(1 - y, z, c), "d2d": dev(y, z, 1 - c)}

    def half(ref, b, h):
        return ref.at[pl.ds(pl.multiple_of(b * R + h * HB, HB), HB), :]

    def block(ref, b):
        return ref.at[pl.ds(pl.multiple_of(b * R, R), R), :]

    barrier = pltpu.get_barrier_semaphore()
    for name in ("in", "y", "d2d"):
        pl.semaphore_signal(barrier, inc=1, device_id=targets[name], device_id_type=pl.DeviceIdType.MESH)

    @pl.when(corner == 0)
    def _():
        pl.semaphore_signal(barrier, inc=1, device_id=targets["out"], device_id_type=pl.DeviceIdType.MESH)

    pl.semaphore_wait(barrier, 4 - corner)

    def ag_copy(a, p, yr, h, link, own):
        yy, zz = place(p, yr)
        b = yy * 8 + zz * 2 + c
        src = own_in[a].at[pl.ds(h * HB, HB), :] if own else half(full[a], b, h)
        return pltpu.make_async_remote_copy(
            src_ref=src, dst_ref=half(full[a], b, h), send_sem=ag_send.at[a, 0 if link in ("in", "out") else 1],
            recv_sem=ag_recv.at[a, b, h], device_id=targets[link], device_id_type=pl.DeviceIdType.MESH)

    def arrived(a, b, h):
        pltpu.make_async_copy(half(full[a], b, h), half(full[a], b, h), ag_recv.at[a, b, h]).wait()

    def service(kind, waits, sends):
        for a, p, yr, h in waits:
            yy, zz = place(p, yr)
            arrived(a, yy * 8 + zz * 2 + c, h)
        for a, p, yr, h, link in sends:
            ag_copy(a, p, yr, h, link, own=(p == OWN[kind] and yr == 0)).start()

    plans = {kind: services(kind) for kind in ("C", "M")}

    def task_t1(q, code, wd, dyb, gb, ub):
        loaded, slot, after = code % 2, (code // 2) % 2, code // 4 - 1

        def loads(q, s):
            b, _ = where(q)
            return (pltpu.make_async_copy(block(dyg, b), dyb.at[s], ld.at[s]),
                    pltpu.make_async_copy(block(gate_ref, b), gb.at[s], ld.at[2 + s]),
                    pltpu.make_async_copy(block(up_ref, b), ub.at[s], ld.at[4 + s]))

        def start(q, s):
            @pl.when(q % 2 == 1)
            def _():
                for h in range(2):
                    arrived(DY, where(q)[0], h)

            for cp in loads(q, s):
                cp.start()

        @pl.when(loaded == 0)
        def _():
            start(q, slot)

        @pl.when(after >= 0)
        def _():
            start(after, 1 - slot)

        here = loads(q, slot)
        here[0].wait()
        acc[:, :C] = lax.dot_general(dyb[slot], wd[...], NT, preferred_element_type=F32)
        for cp in here[1:]:
            cp.wait()
        rc = 32

        @pl.loop(0, R // rc)
        def _(r):
            rs = pl.ds(pl.multiple_of(r * rc, rc), rc)
            to = pl.ds(pl.multiple_of(q * R + r * rc, rc), rc)
            dh, gg, uu = acc[rs, :C], gb[slot, rs, :].astype(F32), ub[slot, rs, :].astype(F32)
            s = jax.nn.sigmoid(gg)
            silu = gg * s
            acc[rs, C:2 * C] = silu * uu
            dgu[to, C:] = (dh * silu).astype(BF)
            dgu[to, :C] = ((dh * uu) * (s * (1.0 + gg * (1.0 - s)))).astype(BF)

        ht[:, pl.ds(pl.multiple_of(q * R, R), R)] = acc[:, C:2 * C].T.astype(BF)

    def product(q, n):
        lhs = dgu[pl.ds(pl.multiple_of(q * R, R), R), :]
        return lax.dot_general(lhs, wgu[pl.ds(pl.multiple_of(n * HN, HN), HN), :], NT, preferred_element_type=F32)

    def cols_of(n):
        return pl.ds(pl.multiple_of(n * HN, HN), HN)

    def od_copy(out_d, u, n):
        return pltpu.make_async_remote_copy(
            src_ref=out_d.at[n], dst_ref=pb.at[u, :, cols_of(n)], send_sem=od_send.at[n], recv_sem=pb_recv.at[u, n],
            device_id=targets["d2d"], device_id_type=pl.DeviceIdType.MESH)

    def task_t2p(q, first, out_d):
        _, u = where(q)

        @pl.loop(0, 2)
        def _(n):
            @pl.when(first == 0)
            def _():
                od_copy(out_d, u, n).wait_send()

            out_d[n] = product(q, n).astype(BF)
            od_copy(out_d, u, n).start()

    def oz_copy(j, n, u, to, dirn):
        return pltpu.make_async_remote_copy(
            src_ref=out_z.at[j % 3, n], dst_ref=rsb.at[dirn, u, :, cols_of(n)], send_sem=oz_send.at[j % 3, n],
            recv_sem=rs_recv.at[dirn, u, n], device_id=dev(y, to, c), device_id_type=pl.DeviceIdType.MESH)

    def y_copy(j, n):
        return pltpu.make_async_remote_copy(
            src_ref=out_z.at[j % 3, n], dst_ref=yb.at[:, cols_of(n)], send_sem=oz_send.at[j % 3, n],
            recv_sem=yb_recv.at[n], device_id=targets["y"], device_id_type=pl.DeviceIdType.MESH)

    def task_t2o(j, n):
        def pick(col, names):
            return jnp.where(is_c, *(table(j, [names.index(e[col]) for e in SUMS[kind]]) for kind in ("C", "M")))

        p, yr, fo, fi = (pick(col, "0123") for col in range(4))
        dest = pick(4, "IOYH")
        q = 8 * yr + 2 * p
        _, u = where(q)
        cs = cols_of(n)
        sources = (
            (jnp.int32(1), pb.at[u, :, cs], pb_recv.at[u, n]),
            (fo, rsb.at[0, u, :, cs], rs_recv.at[0, u, n]),
            (fi, rsb.at[1, u, :, cs], rs_recv.at[1, u, n]),
        )

        def fetch(s):
            flag, ref, sem = sources[s]

            @pl.when(flag == 1)
            def _():
                pltpu.make_async_copy(ref, ref, sem).wait()
                pltpu.make_async_copy(ref, inc.at[s], ld.at[s]).start()

        early = jnp.where((corner == 0) | (j >= 3) | (n == 1), 1, 0)

        @pl.when(early == 1)
        def _():
            fetch(0)

        acc[...] = product(q, n)

        @pl.when(early == 0)
        def _():
            fetch(0)

        fetch(1)
        fetch(2)
        for s, (flag, ref, sem) in enumerate(sources):
            @pl.when(flag == 1)
            def _():
                pltpu.make_async_copy(ref, inc.at[s], ld.at[s]).wait()
                acc[...] += inc[s].astype(F32)

        @pl.when(dest < HERE)
        def _():
            @pl.when(j >= 3)
            def _():
                y_copy(j, n).wait_send()

            out_z[j % 3, n] = acc[...].astype(BF)

        @pl.when(dest < Y)
        def _():
            oz_copy(j, n, u, jnp.where(dest == IN, zin, zout), jnp.where(dest == IN, 1 - corner, 1)).start()

        @pl.when(dest == Y)
        def _():
            y_copy(j, n).start()

        @pl.when(dest == HERE)
        def _():
            done = pltpu.make_async_copy(acc, part_ref.at[:, cs], ld.at[0])
            done.start()
            done.wait()

    def gather(src, q0, count, m, w, buf, s):
        gather_cols(src, where, q0, count, m, w, buf, s, slot_in)

    def task_dwd(lo, hi):
        def body(buf, out):
            def out_copy(m, s):
                return pltpu.make_async_copy(out.at[s], dwd_ref.at[:, pl.ds(pl.multiple_of(m * W, W), W)], slot_out.at[s])

            def work(m, s):
                out[s] = jnp.dot(ht[...], buf[s], preferred_element_type=F32).astype(BF)

            chunks(lo, hi, lambda m, s: gather(dyg, 0, NB, m, W, buf, s),
                   lambda s: pltpu.make_async_copy(buf.at[s], buf.at[s], slot_in.at[s]).wait(), work,
                   lambda m, s: out_copy(m, s).start(), lambda s: out_copy(0, s).wait())

        pl.run_scoped(body, pltpu.VMEM((2, NB * R, W), BF), pltpu.VMEM((2, C, W), BF))

    def x_arrived(q0, count):
        @pl.loop(0, count)
        def _(k):
            b, _ = where(q0 + 2 * k + 1)
            for h in range(2):
                arrived(X, b, h)

    def task_p1(lo, hi):
        @pl.when(lo == 0)
        def _():
            x_arrived(0, 6)

        def body(buf, out):
            def out_copy(m, s):
                return pltpu.make_async_copy(out.at[s], accb.at[pl.ds(pl.multiple_of(m * WP, WP), WP), :], slot_out.at[s])

            def work(m, s):
                out[s] = lax.dot_general(buf[s], dgu[:QA * R, :], TT, preferred_element_type=F32)

            chunks(lo, hi, lambda m, s: gather(xg, 0, QA, m, WP, buf, s),
                   lambda s: pltpu.make_async_copy(buf.at[s], buf.at[s], slot_in.at[s]).wait(), work,
                   lambda m, s: out_copy(m, s).start(), lambda s: out_copy(0, s).wait())

        pl.run_scoped(body, pltpu.VMEM((2, QA * R, WP), BF), pltpu.VMEM((2, WP, 2 * C), F32))

    def task_p3(lo, hi):
        @pl.when(lo == DE // WP)
        def _():
            x_arrived(QA, (NB - QA) // 2)

        def body(buf, out):
            def out_copy(m, s):
                return pltpu.make_async_copy(out.at[s], late_ref.at[pl.ds(pl.multiple_of(m * WP - DE, WP), WP), :], slot_out.at[s])

            def work(m, s):
                out[s] = lax.dot_general(buf[s], dgu[...], TT, preferred_element_type=F32).astype(BF)

            chunks(lo, hi, lambda m, s: gather(xg, 0, NB, m, WP, buf, s),
                   lambda s: pltpu.make_async_copy(buf.at[s], buf.at[s], slot_in.at[s]).wait(), work,
                   lambda m, s: out_copy(m, s).start(), lambda s: out_copy(DE // WP, s).wait())

        pl.run_scoped(body, pltpu.VMEM((2, NB * R, WP), BF), pltpu.VMEM((2, WP, 2 * C), BF))

    def run(phase, handlers):
        steps, at = {"C": [], "M": []}, {}
        points = {kind: steps_of(kind, phase) for kind in steps}
        for n, lists in enumerate(zip(points["C"], points["M"])):
            count = max(1, *map(len, lists))
            at[n + phase * len(TASKS["C"][0])] = len(steps["C"])
            for kind, mine in zip(("C", "M"), lists):
                steps[kind] += mine + [(NONE, 0, 0)] * (count - len(mine))

        @pl.loop(0, len(steps["C"]))
        def _(i):
            for k, start in at.items():
                for kind, mine in kinds.items():
                    waits, sends = (e.get(k, []) for e in plans[kind])
                    if k and (waits or sends):
                        @pl.when((i == start) & mine)
                        def _():
                            service(kind, waits, sends)

            what, a1, a2 = (
                jnp.where(is_c, table(i, [e[col] for e in steps["C"]]), table(i, [e[col] for e in steps["M"]])) for col in range(3))
            for kind, fn in handlers.items():
                @pl.when(what == kind)
                def _():
                    fn(i, a1, a2)

    def phase_one(wd, dyb, gb, ub, out_d):
        for kind, mine in kinds.items():
            @pl.when(mine)
            def _():
                service(kind, *(e.get(0, []) for e in plans[kind]))

        weights = [
            pltpu.make_async_copy(wd_ref, wd, ld.at[3]),
            pltpu.make_async_copy(wg_ref, wgu.at[:, pl.ds(0, C)], ld.at[4]),
            pltpu.make_async_copy(wu_ref, wgu.at[:, pl.ds(C, C)], ld.at[5]),
        ]
        for cp in weights:
            cp.start()
        for a in (DY, X):
            for cp in (pltpu.make_async_copy(own_in[a], dyb.at[0], ld.at[0]), pltpu.make_async_copy(dyb.at[0], block(full[a], t), ld.at[0])):
                cp.start()
                cp.wait()
        for cp in weights:
            cp.wait()
        run(0, {
            T1: lambda i, q, code: task_t1(q, code, wd, dyb, gb, ub),
            T2P: lambda i, q, _: task_t2p(q, jnp.where(i < 3, 1, 0), out_d),
            T2O: lambda i, j, n: task_t2o(j, n),
        })
        for n in range(2):
            od_copy(out_d, 0, n).wait_send()

    pl.run_scoped(phase_one, pltpu.VMEM((C, D), BF), pltpu.VMEM((2, R, D), BF), pltpu.VMEM((2, R, C), BF), pltpu.VMEM((2, R, C), BF),
                  pltpu.VMEM((2, R, HN), BF))
    rest = pltpu.make_async_copy(dgu.at[pl.ds(QA * R, (NB - QA) * R), :], dgq_ref, ld.at[6])
    rest.start()
    run(1, {
        T2O: lambda i, j, n: task_t2o(j, n),
        DWD: lambda i, lo, hi: task_dwd(lo, hi),
        P1: lambda i, lo, hi: task_p1(lo, hi),
        P3: lambda i, lo, hi: task_p3(lo, hi),
    })
    rest.wait()
    for n in range(2):
        pltpu.make_async_copy(yb.at[:, cols_of(n)], yb.at[:, cols_of(n)], yb_recv.at[n]).wait()
        for j in range(3):
            y_copy(j, n).wait_send()
    for kind, mine in kinds.items():
        @pl.when(mine)
        def _():
            sent = [e for es in plans[kind][1].values() for e in es]
            for a in (DY, X):
                for group, links in enumerate((("in", "out"), ("y", "d2d"))):
                    part = full[a].at[pl.ds(0, HB * sum(e[0] == a and e[4] in links for e in sent)), :]
                    pltpu.make_async_copy(part, part, ag_send.at[a, group]).wait()


def finish(part_ref, yb, accb, xg, dgq_ref, dwd_in, late_ref, dx_ref, dwg_ref, dwu_ref, dwd_ref,
           dgq, buf, part, out, mine, theirs, done, late, down, slot_in, acc_in, slot_out, ld, st):
    t = lax.axis_index("tp")
    y, z, c = t // 8, (t // 2) % 4, t % 2
    far = z // 2

    def where(q):
        yr, p, cr = q // 8, (q % 8) // 2, q % 2
        return (y + yr * (1 - 2 * y)) * 8 + (3 * far + (1 - 2 * far) * p) * 2 + c + cr * (1 - 2 * c), 0

    pairs = ((dgq_ref, dgq), (late_ref, late), (dwd_in, down), (part_ref, mine), (yb, theirs))
    loads = [pltpu.make_async_copy(a, b, ld.at[n]) for n, (a, b) in enumerate(pairs)]
    tail = pl.ds(DE, D - DE)
    pairs = ((late.at[:, pl.ds(0, C)], dwg_ref.at[tail, :]), (late.at[:, pl.ds(C, C)], dwu_ref.at[tail, :]), (down, dwd_ref), (done, dx_ref))
    stores = [pltpu.make_async_copy(a, b, st.at[n]) for n, (a, b) in enumerate(pairs)]
    count = DE // W

    def acc_copy(m):
        return pltpu.make_async_copy(accb.at[pl.ds(pl.multiple_of(m * W, W), W), :], part.at[m % 3], acc_in.at[m % 3])

    def start(m):
        gather_cols(xg, where, QA, NB - QA, m, W, buf, m % 3, slot_in)
        acc_copy(m).start()

    def outs(m):
        s, to = m % 2, pl.ds(pl.multiple_of(m * W, W), W)
        return (pltpu.make_async_copy(out.at[s, 0], dwg_ref.at[to, :], slot_out.at[s, 0]),
                pltpu.make_async_copy(out.at[s, 1], dwu_ref.at[to, :], slot_out.at[s, 1]))

    loads[0].start()
    for m in range(2):
        start(m)
    for cp in loads[1:]:
        cp.start()
    loads[0].wait()

    @pl.loop(0, count)
    def _(m):
        s = m % 3

        @pl.when(m + 2 < count)
        def _():
            start(m + 2)

        pltpu.make_async_copy(buf.at[s], buf.at[s], slot_in.at[s]).wait()
        acc_copy(m).wait()

        @pl.when(m >= 2)
        def _():
            for cp in outs(m - 2):
                cp.wait()

        total = part[s] + lax.dot_general(buf[s], dgq[...], TT, preferred_element_type=F32)
        out[m % 2, 0] = total[:, :C].astype(BF)
        out[m % 2, 1] = total[:, C:].astype(BF)
        for cp in outs(m):
            cp.start()

        @pl.when(m == 0)
        def _():
            loads[1].wait()
            for cp in stores[:2]:
                cp.start()

        @pl.when(m == 1)
        def _():
            loads[2].wait()
            stores[2].start()

        @pl.when(m == 2)
        def _():
            for cp in loads[3:]:
                cp.wait()
            done[...] = (mine[...] + theirs[...].astype(F32)).astype(BF)
            stores[3].start()

    for m in range(2):
        for cp in outs(count - 2 + m):
            cp.wait()
    for cp in stores:
        cp.wait()


def solution(mesh):
    def step(x, dy, gate, up, w_gate, w_up, w_down):
        hbm = pl.BlockSpec(memory_space=pl.ANY)
        S = jax.ShapeDtypeStruct
        dma = pltpu.SemaphoreType.DMA
        part, dgq, dwd, late, _, xg, _, _, yb, accb = pl.pallas_call(
            kernel,
            out_shape=[
                S((R, D), F32), S(((NB - QA) * R, 2 * C), BF), S((C, D), BF), S((D - DE, 2 * C), BF),
                S((NB * R, D), BF), S((NB * R, D), BF), S((2, 8, R, D), BF), S((8, R, D), BF), S((R, D), BF),
                S((DE, 2 * C), F32),
            ],
            in_specs=[hbm] * 7,
            out_specs=[hbm] * 10,
            scratch_shapes=[
                pltpu.VMEM((D, 2 * C), BF),
                pltpu.VMEM((NB * R, 2 * C), BF),
                pltpu.VMEM((C, NB * R), BF),
                pltpu.VMEM((3, 2, R, HN), BF),
                pltpu.VMEM((R, HN), F32),
                pltpu.VMEM((3, R, HN), BF),
                dma((2, NB, 2)), dma((2, 2)), dma((2, 8, 2)), dma((8, 2)), dma((2,)), dma((2,)), dma((3, 2)), dma((7,)), dma((2,)),
                dma((2,)),
            ],
            compiler_params=pltpu.CompilerParams(collective_id=0, has_side_effects=True, vmem_limit_bytes=LIMIT),
            name="gather_and_sum",
        )(x, dy, gate, up, w_gate, w_up, w_down)
        return pl.pallas_call(
            finish,
            out_shape=[S((R, D), BF), S((D, C), BF), S((D, C), BF), S((C, D), BF)],
            in_specs=[hbm] * 7,
            out_specs=[hbm] * 4,
            scratch_shapes=[
                pltpu.VMEM(((NB - QA) * R, 2 * C), BF),
                pltpu.VMEM((3, (NB - QA) * R, W), BF),
                pltpu.VMEM((3, W, 2 * C), F32),
                pltpu.VMEM((2, 2, W, C), BF),
                pltpu.VMEM((R, D), F32),
                pltpu.VMEM((R, D), BF),
                pltpu.VMEM((R, D), BF),
                pltpu.VMEM((D - DE, 2 * C), BF),
                pltpu.VMEM((C, D), BF),
                dma((3,)), dma((3,)), dma((2, 2)), dma((5,)), dma((4,)),
            ],
            compiler_params=pltpu.CompilerParams(vmem_limit_bytes=LIMIT),
            name="finish",
        )(part, yb, accb, xg, dgq, dwd, late)

    rows, cols = P(("dp", "tp"), None), P("dp", "tp")
    return jax.shard_map(
        step,
        mesh=mesh,
        in_specs=(rows, rows, cols, cols, P(None, "tp"), P(None, "tp"), P("tp", None)),
        out_specs=(rows, cols, cols, rows),
        check_vma=False,
    )
```
